32 devices in a mesh: blk: 8 (over z, x), rows: 4 (over y, core).
Axes of the slice: x: 2, y: 2, z: 4, core: 2. Of those that a mesh axis runs over, the one named last changes fastest.
Arguments:
- columns: float32 [512, 16384], P('blk', 'rows'), may hold values from -100 to 100
- plan: int32 [3, 16], replicated, may hold values from 0 to 15, as said below
Outputs:
- swept: float32 [512, 16384], P('blk', 'rows')
- off_ratio: float32 [3], replicated
The draws below stay inside these ranges and needn't reach their ends.
Inputs may be any that keep to these rules, and one draw needn't show every extreme that they name: `plan`: row s is a permutation of the 16 positions (position k is slot k % 2 of blk index k // 2). In each row there are a slot t and a number m of 1 to 7 such that the block in slot t of every blk index i goes to slot t of blk index (i + m) modulo 16 / 2, and every other block stays where it is.
All inputs are finite; a program needn't handle non-finite values. Where the reference program divides by a largest or mean magnitude, that divisor is 1e-20 or more.
Results may differ from the reference program's by a relative error of at most 0.00011.
Values sent between devices are 32-bit elements; how exact they have to be, the bound alone decides.
A program may use at most 64 MiB of HBM per device.

```python
import math
import jax
import jax.numpy as jnp
from jax import lax

BW = 32
STEPS = 3
EIG_ITERS = 3
NS_ITERS = 8
BLOCKS = 16
NCOL = 512
M = 16384


def draw_columns(key, part):
    keys = jax.random.split(jax.random.fold_in(key, 11), 2)
    position = jnp.arange(NCOL, dtype=jnp.float32) / NCOL
    scales = jnp.exp(jax.random.uniform(keys[0], (NCOL,), jnp.float32, 0.0, math.log(6.0)))
    entries = jax.random.normal(keys[1], (NCOL, M), jnp.float32)
    trend = 1.0 + 0.8 * position
    values = entries * (scales * trend)[:, None]
    return jnp.clip(values, -100.0, 100.0).astype(jnp.float32)


def draw_plan(key, part):
    keys = jax.random.split(jax.random.fold_in(key, 23), 2)
    half = BLOCKS // 2
    partner_steps = jax.random.randint(keys[0], (STEPS,), 1, half)
    leaving_slots = jax.random.randint(keys[1], (STEPS,), 0, 2)
    position = jnp.arange(BLOCKS, dtype=jnp.int32)
    device_index = position // 2
    slot_index = position % 2
    moved = (device_index[None, :] + partner_steps[:, None]) % half * 2 + slot_index[None, :]
    table = jnp.where(slot_index[None, :] == leaving_slots[:, None], moved, position[None, :])
    return table.astype(jnp.int32)


def setup_inputs(seed: int = 0) -> dict:
    key_of = jax.random.split(jax.random.key(seed), 3)
    return {
        "columns": draw_columns(jax.random.fold_in(key_of[2], 71), 0),
        "plan": draw_plan(jax.random.fold_in(key_of[2], 71), 0),
    }


PRECISE = lax.Precision.HIGHEST

def matmul(left, right):
    return jnp.matmul(left, right, precision=PRECISE, preferred_element_type=jnp.float32)

def flipped(matrix):
    return jnp.swapaxes(matrix, -1, -2)

def orthonormal(matrix):
    lengths = jnp.sqrt(lax.optimization_barrier(jnp.sum(matrix * matrix, axis=-2, keepdims=True)))
    normed = matrix / lengths
    inner = matmul(flipped(normed), normed)
    bound = lax.optimization_barrier(jnp.max(lax.optimization_barrier(jnp.sum(jnp.abs(inner), axis=-1)), axis=-1))
    normed = normed / jnp.sqrt(bound)[..., None, None]
    for turn_index in range(NS_ITERS):
        normed = 1.5 * normed - 0.5 * matmul(normed, matmul(flipped(normed), normed))
    return normed

def pair_rotation(gram_sum):
    rotation = jnp.broadcast_to(jnp.eye(gram_sum.shape[-1], dtype=gram_sum.dtype), gram_sum.shape)
    for turn_index in range(EIG_ITERS):
        rotation = orthonormal(matmul(gram_sum, rotation))
    return rotation

def reference(columns, plan):
    current = columns
    eye_mask = jnp.eye(2 * BW, dtype=bool)
    ratios = []
    for step_index in range(STEPS):
        pairs = current.reshape(BLOCKS // 2, 2 * BW, M)
        gram_sum = matmul(pairs, flipped(pairs))
        off_part = jnp.where(eye_mask, 0.0, gram_sum)
        diag_part = jnp.where(eye_mask, gram_sum, 0.0)
        off_total = jnp.sum(off_part * off_part)
        diag_total = jnp.sum(diag_part * diag_part)
        ratios.append(jnp.sqrt(off_total) / jnp.sqrt(diag_total))
        rotation = pair_rotation(gram_sum)
        rotated = matmul(flipped(rotation), pairs)
        blocks = rotated.reshape(BLOCKS, BW, M)
        placed = jnp.zeros_like(blocks).at[plan[step_index]].set(blocks)
        current = placed.reshape(NCOL, M)
    return (current, jnp.stack(ratios))
```

```python
from functools import partial

import jax
import jax.numpy as jnp
from jax import lax
from jax.experimental import pallas as pl
from jax.experimental.pallas import tpu as pltpu
from jax.sharding import PartitionSpec as P

EIG_ITERS = 3
NS_ITERS = 8
UNROLLED = 8
MESH = pl.DeviceIdType.MESH
(EXCHANGE, EXCHANGE_LATE, TURN0, DIAG0, PARTS, CROSS, LEAD1, DIAG1, STAY1, TURN2, STATS,
 SPREAD, SPREAD_MORE, MIRROR, MIRROR_MORE, NEAR, NEAR_MORE, FAR) = range(18)
BLK_PHASES = 18
ROW_SUMS = 3
ROW_PHASES = 4


def split(value):
    high = value.astype(jnp.bfloat16)
    low = (value - high.astype(jnp.float32)).astype(jnp.bfloat16)
    return high, low


def left_of(value):
    high = value.astype(jnp.bfloat16).astype(jnp.float32)
    low = value - high
    lane = lax.broadcasted_iota(jnp.int32, value.shape, 1)
    mixed = jnp.where(lane < value.shape[1] // 2, high, low).astype(jnp.bfloat16)
    return jnp.concatenate([mixed, mixed], axis=1)


def right_of(value):
    high, low = split(value)
    return jnp.concatenate([high, high, low, low], axis=0)


def turned_right_of(value):
    high, low = split(value)
    both = jnp.concatenate([high, low], axis=1)
    return jnp.concatenate([both, both], axis=0)


def dot(left, right):
    return jnp.dot(left, right, preferred_element_type=jnp.float32)


def dot_turned(left, right):
    return lax.dot_general(left, right, (((1,), (1,)), ((), ())), preferred_element_type=jnp.float32)


def cross_gram(first, second):
    width = first.shape[0]
    left = jnp.concatenate(split(first), axis=0)
    right = left if second is first else jnp.concatenate(split(second), axis=0)
    products = dot_turned(left, right)
    folded = products + pltpu.roll(products, width, 1)
    return folded[:width] + folded[width:]


def lane_of(value):
    return lax.broadcasted_iota(jnp.int32, value.shape, 1)


def pack(value):
    half = value.shape[0] // 2
    top = value[:half]
    return jnp.where(lane_of(top) < value.shape[1] // 2, top, value[half:])


def unpack(packed):
    width = packed.shape[1] // 2
    turned = pltpu.roll(packed, width, 1)
    first = lane_of(packed) < width
    return jnp.where(first, packed, turned), jnp.where(first, turned, packed)


def block_cross(first, second):
    half = first.shape[0]
    high, low = split(second)
    right = jnp.concatenate([high, low, high, low], axis=0)
    products = dot_turned(jnp.concatenate(split(first), axis=0), right)
    folded = products + pltpu.roll(products, half, 1)
    return folded[:half] + folded[half:]


def pack_block(value):
    half, across = value.shape
    groups = across // half
    rows = half // groups
    packed = value[:rows]
    for index in range(1, groups):
        packed = jnp.where(lane_of(packed) < index * half, packed, value[index * rows:(index + 1) * rows])
    return packed


def unpack_block(packed, half):
    groups = packed.shape[1] // half
    lane = lane_of(packed)
    rows = []
    for index in range(groups):
        value = jnp.where((lane >= index * half) & (lane < (index + 1) * half), packed, 0.0)
        reach = half
        while reach < packed.shape[1]:
            value = value + pltpu.roll(value, reach, 1)
            reach *= 2
        rows.append(value)
    return jnp.concatenate(rows, axis=0)


def flip_block(value):
    half, across = value.shape
    return jnp.concatenate([value] * (across // half), axis=0).T[:half]


def orthonormal(z, zt):
    y = z / jnp.sqrt(jnp.sum(z * z, axis=0, keepdims=True))
    t = zt / jnp.sqrt(0.5 * jnp.sum(zt * zt, axis=1, keepdims=True))
    inner = dot(left_of(t), right_of(y))
    bound = jnp.max(jnp.sum(jnp.abs(inner), axis=0, keepdims=True), axis=1, keepdims=True)
    root = jnp.sqrt(bound)
    y = y / root
    t = t / root

    def finish(y, t, inner):
        y_next = 1.5 * y - 0.5 * dot(left_of(y), right_of(inner))
        t_next = 1.5 * t - 0.5 * dot(left_of(inner), right_of(t))
        return y_next, t_next

    def turn(_, carry):
        y, t = carry
        return finish(y, t, dot(left_of(t), right_of(y)))

    return lax.fori_loop(1, NS_ITERS, turn, finish(y, t, inner / bound))


def pair_rotation(gram):
    q, t = orthonormal(gram, gram)
    gram_left, gram_right = left_of(gram), right_of(gram)

    def again(_, carry):
        q, t = carry
        return orthonormal(dot(gram_left, right_of(q)), dot(left_of(t), gram_right))

    return lax.fori_loop(1, EIG_ITERS, again, (q, t))[1]


def each(count, body):
    if count <= UNROLLED:
        for index in range(count):
            body(index)
    else:
        def loop(index, carry):
            body(index)
            return carry
        lax.fori_loop(0, count, loop, 0)


def totals(gram, seen, step):
    width = gram.shape[0]
    row = lax.broadcasted_iota(jnp.int32, gram.shape, 0)
    column = lane_of(gram)
    square = gram * gram
    diag_part = jnp.where(row == column, square, 0.0)
    off_part = jnp.where((row == column) | (column >= width), 0.0, square)
    off_total = jnp.sum(jnp.sum(off_part, axis=0, keepdims=True), axis=1, keepdims=True)
    diag_total = jnp.sum(jnp.sum(diag_part, axis=0, keepdims=True), axis=1, keepdims=True)
    line = lax.broadcasted_iota(jnp.int32, seen.shape, 0)
    fresh = jnp.where(line == 0, off_total, diag_total)
    return jnp.where((lane_of(seen) == step) & (line < 2), fresh, seen)


def doubled(lanes):
    return lanes // 2 // 256 * 256


def kernel(plan_hbm, columns_ref, out_ref, stat_ref,
           plan_ref, columns, raw, turned, paired, ready, extra_raw, extra, extra_paired, own_turn, quarters, leads, stays, last_turns,
           parts, part_in, part_sums, diags, more_diags, crosses, cross_in, sums, stats,
           plan_sem, fetch_sem, blk_send, blk_recv, row_send, row_recv):
    width, share = columns.shape
    half = width // 2
    count = lax.axis_size("rows")
    others = lax.axis_size("blk")
    me = lax.axis_index("rows")
    mine = lax.axis_index("blk")
    lanes = share // others
    early = lanes // 2 // 128 * 128
    quarter = quarters.shape[2]
    shared = doubled(lanes)
    kept = lanes - shared
    group = others // 2
    base = mine // group * group
    mirror_base = group - base
    place = mine - base
    far_first = sorted(range(1, others), key=lambda offset: (abs(2 * offset - others), offset))

    fetch = pltpu.make_async_copy(columns_ref, columns, fetch_sem)
    fetch.start()
    plan_fetch = pltpu.make_async_copy(plan_hbm, plan_ref, plan_sem)
    plan_fetch.start()
    barrier = pltpu.get_barrier_semaphore()
    for offset in range(1, count):
        pl.semaphore_signal(barrier, inc=1, device_id={"rows": lax.rem(me + offset, count)}, device_id_type=MESH)
    for offset in range(1, others):
        pl.semaphore_signal(barrier, inc=1, device_id={"blk": lax.rem(mine + offset, others)}, device_id_type=MESH)

    def peer_of(offset):
        return lax.rem(mine + offset, others)

    def send(phase, slot, peer, src, dst):
        copy = pltpu.make_async_remote_copy(
            src_ref=src, dst_ref=dst,
            send_sem=blk_send.at[phase, slot], recv_sem=blk_recv.at[phase, slot],
            device_id={"blk": peer}, device_id_type=MESH)
        copy.start()
        return copy

    def blk_copy(phase, offset, src, dst):
        return send(phase, offset - 1, peer_of(offset), src, dst)

    def near_peer(offset):
        return base + lax.rem(place + offset, group)

    def far_peer(offset):
        return mirror_base + lax.rem(place + offset, group)

    def gather(phase, ref):
        return [blk_copy(phase, offset, ref.at[mine], ref.at[mine]) for offset in far_first]

    def scatter(phase, src_ref, dst_ref):
        return [blk_copy(phase, offset, src_ref.at[peer_of(offset)], dst_ref.at[mine]) for offset in far_first]

    def exchange(phase, src_ref, start, size):
        copies = []
        for offset in far_first:
            lane_start = pl.multiple_of(peer_of(offset) * lanes + start, 128)
            copies.append(blk_copy(phase, offset, src_ref.at[:, pl.ds(lane_start, size)],
                                   raw.at[mine, :, pl.ds(start, size)]))
        return copies

    def finish(copies):
        for copy in copies:
            copy.wait()

    def total_of(ref):
        total = ref[0]
        for index in range(1, ref.shape[0]):
            total = total + ref[index]
        return total

    def share_rows(phase, ref):
        copies = []
        for offset in range(1, count):
            copy = pltpu.make_async_remote_copy(
                src_ref=ref.at[me], dst_ref=ref.at[me],
                send_sem=row_send.at[phase, offset - 1], recv_sem=row_recv.at[phase, offset - 1],
                device_id={"rows": lax.rem(me + offset, count)}, device_id_type=MESH)
            copy.start()
            copies.append(copy)
        return copies

    def start_rows(phase, packed):
        sums[phase, me] = packed
        return share_rows(phase, sums.at[phase])

    def end_rows(phase, copies):
        finish(copies)
        return total_of(sums.at[phase])

    def source(step, slot, pair):
        return lax.rem(pair + others - (plan_ref[step, slot] >> 1), others)

    def partner(step):
        return lax.rem(mine + others - (plan_ref[step, 0] >> 1) - (plan_ref[step, 1] >> 1), others)

    def placed(ref, step, pair, where=slice(None)):
        return jnp.concatenate([ref[source(step, 0, pair), pl.ds(0, half), where],
                                ref[source(step, 1, pair), pl.ds(half, half), where]], axis=0)

    def whole(packed):
        return jnp.concatenate(unpack(packed), axis=0)

    low_lane = (lax.broadcasted_iota(jnp.int32, (half, 2 * width), 1) & (width - 1)) < half
    def rotated_diag(turn, gram, first_leaves):
        rotated = dot_turned(left_of(dot(left_of(turn), right_of(gram))), turned_right_of(turn))
        first, second = rotated[:half], rotated[half:]
        leaving = jnp.where(first_leaves,
                            jnp.where(low_lane, first, pltpu.roll(first, half, 1)),
                            jnp.where(low_lane, pltpu.roll(second, half, 1), second))
        return first, second, pack_block(leaving)

    def spread(more):
        size = shared // 2
        start = kept + more * size
        into = pl.ds(more * size, size)
        copies = []
        for offset in range(1, group):
            peer = near_peer(offset)
            mirrored = mirror_base + peer - base
            lane_start = pl.multiple_of(mirrored * lanes + start, 128)
            copies.append(send(SPREAD + more, offset - 1, peer, columns.at[:, pl.ds(lane_start, size)],
                               extra_raw.at[mine, :, into]))
        copies.append(send(MIRROR + more, 0, mirror_base + place, raw.at[pl.ds(base, group), :, pl.ds(start, size)],
                           extra_raw.at[pl.ds(base, group), :, into]))
        lane_start = pl.multiple_of((mirror_base + place) * lanes + start, 128)
        extra_raw[mine, :, into] = columns[:, pl.ds(lane_start, size)]
        return copies

    pl.semaphore_wait(barrier, count - 1 + others - 1)
    early_copies = exchange(EXCHANGE, columns_ref, 0, early) if early else []
    fetch.wait()
    value = columns[...]
    gram = cross_gram(value, value)
    row_copies = start_rows(0, pack(gram))
    raw[mine] = columns[:, pl.ds(pl.multiple_of(mine * lanes, 128), lanes)]
    plan_fetch.wait()

    gram = whole(end_rows(0, row_copies))
    seen = totals(gram, jnp.zeros(stats.shape[1:], jnp.float32), 0)
    turn = pair_rotation(gram)
    own_turn[...] = pack(turn)
    my_quarter = pl.ds(pl.multiple_of(me * quarter, quarter), quarter)
    turn_copies = [blk_copy(TURN0, offset, own_turn.at[my_quarter], quarters.at[me, mine]) for offset in far_first]
    late_copies = exchange(EXCHANGE_LATE, columns, early, lanes - early)
    first_leaves = (plan_ref[0, 0] >> 1) > 0
    first_diag, second_diag, diags[mine] = rotated_diag(turn, gram, first_leaves)
    diag_copies = gather(DIAG0, diags)
    quarters[me, mine] = own_turn[my_quarter]
    finish(turn_copies)
    turn_rows = share_rows(ROW_SUMS, quarters)
    finish(turn_rows)

    def first_turn_of(pair):
        return whole(jnp.concatenate([quarters[index, pair] for index in range(count)], axis=0))

    def first_turn(start, size):
        def body(pair):
            where = pl.ds(start, size)
            turned[pair, :, where] = dot(left_of(first_turn_of(pair)), right_of(raw[pair, :, where]))
        each(others, body)

    finish(early_copies)
    if early:
        first_turn(0, early)
    finish(late_copies)
    first_turn(early, lanes - early)

    def pair_gram(pair):
        value = placed(turned, 0, pair)
        paired[pair] = value
        parts[pair] = pack_block(block_cross(value[:half], value[half:]))

    each(others, pair_gram)
    part_copies = scatter(PARTS, parts, part_in)
    part_in[mine] = parts[mine]

    def pair_cross(pair):
        crosses[pair] = pack(cross_gram(paired[source(1, 0, pair)], paired[source(1, 1, pair)]))

    each(others, pair_cross)
    cross_in[mine] = crosses[mine]

    finish(part_copies)
    part_sums[me] = total_of(part_in)
    row_copies = share_rows(1, part_sums)
    cross_copies = scatter(CROSS, crosses, cross_in)
    finish(diag_copies)
    from_other = unpack_block(diags[partner(0)], half)
    finish(row_copies)
    block = unpack_block(total_of(part_sums), half)
    gram = jnp.concatenate([
        jnp.where(low_lane, jnp.where(first_leaves, from_other, first_diag), block),
        jnp.where(low_lane, flip_block(block), jnp.where(first_leaves, second_diag, from_other))], axis=0)
    spread_copies = spread(0) if shared else []
    seen = totals(gram, seen, 1)
    turn = pair_rotation(gram)
    first_leaves = (plan_ref[1, 0] >> 1) > 0
    lead = jnp.where(first_leaves, turn[:half], turn[half:])
    stay = jnp.where(first_leaves, turn[half:], turn[:half])
    leads[mine] = pack(lead)
    lead_copies = gather(LEAD1, leads)
    stays[mine] = pack(stay)
    first_diag, second_diag, more_diags[mine] = rotated_diag(turn, gram, first_leaves)
    diag_copies = gather(DIAG1, more_diags)
    finish(cross_copies)
    cross_rows = start_rows(2, total_of(cross_in))
    cross = whole(end_rows(2, cross_rows))
    cross_right, cross_turned = right_of(cross), turned_right_of(cross)
    finish(lead_copies)
    from_other = whole(leads[partner(1)])
    first_turns = jnp.where(first_leaves, from_other, stay)
    second_turns = jnp.where(first_leaves, stay, from_other)
    inner = jnp.concatenate([dot(left_of(first_turns), cross_right),
                             dot_turned(left_of(second_turns), cross_turned)], axis=0)
    outer = dot_turned(left_of(inner), turned_right_of(jnp.concatenate([first_turns, second_turns], axis=0)))
    finish(diag_copies)
    stay_copies = gather(STAY1, stays)
    finish(spread_copies)
    spread_copies = spread(1) if shared else []
    from_other = unpack_block(more_diags[partner(1)], half)
    gram = jnp.concatenate([
        jnp.where(low_lane, jnp.where(first_leaves, from_other, first_diag), outer[:half]),
        jnp.where(low_lane, outer[half:], jnp.where(first_leaves, second_diag, from_other))], axis=0)
    stats[mine] = totals(gram, seen, 2)
    stat_copies = gather(STATS, stats)
    last_turns[mine] = pack(pair_rotation(gram))
    turn_copies = gather(TURN2, last_turns)

    finish(stay_copies)

    def second_turn_of(pair):
        lead, stay = whole(leads[pair]), whole(stays[pair])
        return left_of(jnp.concatenate([jnp.where(first_leaves, lead, stay),
                                        jnp.where(first_leaves, stay, lead)], axis=0))

    def second_turn(pair):
        ready[pair] = dot(second_turn_of(pair), right_of(paired[pair]))

    each(others, second_turn)

    def pair_again(pair):
        paired[pair] = placed(ready, 1, pair)

    each(others, pair_again)
    finish(spread_copies)
    if shared:
        def extra_first(pair):
            extra[pair] = dot(left_of(first_turn_of(pair)), right_of(extra_raw[pair]))

        def extra_pair(pair):
            extra_paired[pair] = placed(extra, 0, pair)

        def extra_second(pair):
            extra_raw[pair] = dot(second_turn_of(pair), right_of(extra_paired[pair]))

        def extra_again(pair):
            extra_paired[pair] = placed(extra_raw, 1, pair)

        each(others, extra_first)
        each(others, extra_pair)
        each(others, extra_second)
        each(others, extra_again)
    finish(stat_copies)
    total = total_of(stats)
    stat_ref[...] = jnp.broadcast_to(jnp.sqrt(total[0:1]) / jnp.sqrt(total[1:2]), stat_ref.shape)
    finish(turn_copies)

    def last_turn(pair, ref, size):
        first, second = source(2, 0, pair), source(2, 1, pair)
        where = pl.ds(0, size)
        upper = dot(left_of(unpack(last_turns[first])[0]), right_of(ref[first, :, where]))
        lower = dot(left_of(unpack(last_turns[second])[1]), right_of(ref[second, :, where]))
        return jnp.concatenate([upper, lower], axis=0)

    def lanes_at(chunk, start, size):
        return pl.ds(pl.multiple_of(chunk * lanes + start, 128), size)

    back = []
    for offset in range(group):
        peer = far_peer(offset)
        turned[peer, :, pl.ds(0, kept)] = last_turn(peer, paired, kept)
        back.append(send(FAR, offset, peer, turned.at[peer, :, pl.ds(0, kept)], out_ref.at[:, lanes_at(mine, 0, kept)]))
    mirror = mirror_base + place
    for offset in list(range(1, group)) + [0]:
        peer = near_peer(offset)
        result = last_turn(peer, paired, lanes)
        if offset:
            turned[peer] = result
            back.append(send(NEAR, offset - 1, peer, turned.at[peer], out_ref.at[:, lanes_at(mine, 0, lanes)]))
        else:
            out_ref[:, lanes_at(mine, 0, lanes)] = result
        if shared:
            result = last_turn(peer, extra_paired, shared)
            if offset:
                extra[peer] = result
                back.append(send(NEAR_MORE, offset - 1, peer, extra.at[peer],
                                 out_ref.at[:, lanes_at(mirror, kept, shared)]))
            else:
                out_ref[:, lanes_at(mirror, kept, shared)] = result
    finish(back)


def place_kernel(current_ref, stat_ref, out_ref, ratio_ref, sems):
    width = current_ref.shape[0]
    pieces = sems.shape[0]
    size = width // pieces
    copies = []
    for index in range(pieces):
        where = pl.ds(index * size, size)
        copy = pltpu.make_async_copy(current_ref.at[where], out_ref.at[where], sems.at[index])
        copy.start()
        copies.append(copy)
    line = lax.broadcasted_iota(jnp.int32, stat_ref.shape, 0)
    values = stat_ref[...]
    for index in range(ratio_ref.shape[0]):
        ratio_ref[index] = jnp.sum(jnp.where((lane_of(values) == index) & (line == 0), values, 0.0))
    for copy in copies:
        copy.wait()


def local(columns, plan):
    width, share = columns.shape
    half = width // 2
    steps = plan.shape[0]
    count = lax.axis_size("rows")
    others = lax.axis_size("blk")
    lanes = share // others
    smem = pl.BlockSpec(memory_space=pltpu.SMEM)
    vmem = pl.BlockSpec(memory_space=pltpu.VMEM)
    hbm = pl.BlockSpec(memory_space=pl.ANY)
    stored = pl.BlockSpec(memory_space=pltpu.HBM)
    wide = pltpu.VMEM((others, width, lanes), jnp.float32)
    more = pltpu.VMEM((others, width, max(doubled(lanes), 128)), jnp.float32)
    small = pltpu.VMEM((others, half, 2 * width), jnp.float32)
    smaller = pltpu.VMEM((others, half // 2, 2 * width), jnp.float32)
    block = pltpu.VMEM((others, half * half // (2 * width), 2 * width), jnp.float32)
    current, stat = pl.pallas_call(
        kernel,
        out_shape=(
            jax.ShapeDtypeStruct(columns.shape, jnp.float32),
            jax.ShapeDtypeStruct((8, 128), jnp.float32),
        ),
        in_specs=[stored, stored],
        out_specs=(vmem, vmem),
        scratch_shapes=[
            pltpu.SMEM(plan.shape, jnp.int32),
            pltpu.VMEM((width, share), jnp.float32),
            wide, wide, wide, wide,
            more, more, more,
            pltpu.VMEM((half, 2 * width), jnp.float32),
            pltpu.VMEM((count, others, half // count, 2 * width), jnp.float32),
            smaller, smaller, small,
            block, block, pltpu.VMEM((count,) + block.shape[1:], jnp.float32), block, block,
            small, small,
            pltpu.VMEM((ROW_SUMS, count, half, 2 * width), jnp.float32),
            pltpu.VMEM((others, 8, 128), jnp.float32),
            pltpu.SemaphoreType.DMA,
            pltpu.SemaphoreType.DMA,
            pltpu.SemaphoreType.DMA((BLK_PHASES, max(others - 1, 1))),
            pltpu.SemaphoreType.DMA((BLK_PHASES, max(others - 1, 1))),
            pltpu.SemaphoreType.DMA((ROW_PHASES, max(count - 1, 1))),
            pltpu.SemaphoreType.DMA((ROW_PHASES, max(count - 1, 1))),
        ],
        compiler_params=pltpu.CompilerParams(collective_id=0, has_side_effects=True, vmem_limit_bytes=24 << 20),
        name="steps",
    )(plan, columns)
    return pl.pallas_call(
        place_kernel,
        out_shape=(
            jax.ShapeDtypeStruct(columns.shape, jnp.float32),
            jax.ShapeDtypeStruct((steps,), jnp.float32),
        ),
        in_specs=[vmem, vmem],
        out_specs=(hbm, smem),
        scratch_shapes=[pltpu.SemaphoreType.DMA((8,))],
        compiler_params=pltpu.CompilerParams(vmem_limit_bytes=8 << 20),
        name="place",
    )(current, stat)


def solution(mesh):
    return jax.shard_map(
        local,
        mesh=mesh,
        in_specs=(P("blk", "rows"), P()),
        out_specs=(P("blk", "rows"), P()),
        check_vma=False,
    )
```

```python
from functools import partial

import jax
import jax.numpy as jnp
from jax import lax
from jax.experimental import pallas as pl
from jax.experimental.pallas import tpu as pltpu
from jax.sharding import PartitionSpec as P

EIG_ITERS = 3
NS_ITERS = 8
UNROLLED = 8
AHEAD = 1
MESH = pl.DeviceIdType.MESH
(EXCHANGE, EXCHANGE_LATE, TURN0, DIAG0, PARTS, CROSS, LEAD1, DIAG1, STAY1, TURN2, STATS,
 SPREAD, SPREAD_MORE, MIRROR, MIRROR_MORE, NEAR, NEAR_MORE, FAR) = range(18)
BLK_PHASES = 18
ROW_SUMS = 3
ROW_PHASES = 4


def split(value):
    high = value.astype(jnp.bfloat16)
    low = (value - high.astype(jnp.float32)).astype(jnp.bfloat16)
    return high, low


def left_of(value):
    high = value.astype(jnp.bfloat16).astype(jnp.float32)
    low = value - high
    lane = lax.broadcasted_iota(jnp.int32, value.shape, 1)
    mixed = jnp.where(lane < value.shape[1] // 2, high, low).astype(jnp.bfloat16)
    return jnp.concatenate([mixed, mixed], axis=1)


def right_of(value):
    high, low = split(value)
    return jnp.concatenate([high, high, low, low], axis=0)


def turned_right_of(value):
    high, low = split(value)
    both = jnp.concatenate([high, low], axis=1)
    return jnp.concatenate([both, both], axis=0)


def dot(left, right):
    return jnp.dot(left, right, preferred_element_type=jnp.float32)


def dot_turned(left, right):
    return lax.dot_general(left, right, (((1,), (1,)), ((), ())), preferred_element_type=jnp.float32)


def cross_gram(first, second):
    width = first.shape[0]
    left = jnp.concatenate(split(first), axis=0)
    right = left if second is first else jnp.concatenate(split(second), axis=0)
    products = dot_turned(left, right)
    folded = products + pltpu.roll(products, width, 1)
    return folded[:width] + folded[width:]


def lane_of(value):
    return lax.broadcasted_iota(jnp.int32, value.shape, 1)


def pack(value):
    half = value.shape[0] // 2
    top = value[:half]
    return jnp.where(lane_of(top) < value.shape[1] // 2, top, value[half:])


def unpack(packed):
    width = packed.shape[1] // 2
    turned = pltpu.roll(packed, width, 1)
    first = lane_of(packed) < width
    return jnp.where(first, packed, turned), jnp.where(first, turned, packed)


def block_cross(first, second):
    half = first.shape[0]
    high, low = split(second)
    right = jnp.concatenate([high, low, high, low], axis=0)
    products = dot_turned(jnp.concatenate(split(first), axis=0), right)
    folded = products + pltpu.roll(products, half, 1)
    return folded[:half] + folded[half:]


def pack_block(value):
    half, across = value.shape
    groups = across // half
    rows = half // groups
    packed = value[:rows]
    for index in range(1, groups):
        packed = jnp.where(lane_of(packed) < index * half, packed, value[index * rows:(index + 1) * rows])
    return packed


def unpack_block(packed, half):
    groups = packed.shape[1] // half
    lane = lane_of(packed)
    rows = []
    for index in range(groups):
        value = jnp.where((lane >= index * half) & (lane < (index + 1) * half), packed, 0.0)
        reach = half
        while reach < packed.shape[1]:
            value = value + pltpu.roll(value, reach, 1)
            reach *= 2
        rows.append(value)
    return jnp.concatenate(rows, axis=0)


def flip_block(value):
    half, across = value.shape
    return jnp.concatenate([value] * (across // half), axis=0).T[:half]


def orthonormal(z, zt, gram_left, gram_right):
    y = z / jnp.sqrt(jnp.sum(z * z, axis=0, keepdims=True))
    t = zt / jnp.sqrt(0.5 * jnp.sum(zt * zt, axis=1, keepdims=True))
    inner = dot(left_of(t), right_of(y))
    bound = jnp.max(jnp.sum(jnp.abs(inner), axis=0, keepdims=True), axis=1, keepdims=True)
    root = jnp.sqrt(bound)
    y = y / root
    t = t / root

    def finish(y, t, inner):
        y_next = 1.5 * y - 0.5 * dot(left_of(y), right_of(inner))
        t_next = 1.5 * t - 0.5 * dot(left_of(inner), right_of(t))
        return y_next, t_next

    y, t = finish(y, t, inner / bound)
    for _ in range(2, NS_ITERS):
        y, t = finish(y, t, dot(left_of(t), right_of(y)))
    inner = dot(left_of(t), right_of(y))
    return y, t, inner, finish(dot(gram_left, right_of(y)), dot(left_of(t), gram_right), inner)


def pair_rotation(gram):
    gram_left, gram_right = left_of(gram), right_of(gram)

    def again(_, carry):
        return orthonormal(*carry, gram_left, gram_right)[3]

    z, zt = lax.fori_loop(1, EIG_ITERS, again, (gram, gram))
    y, t, inner, _ = orthonormal(z, zt, gram_left, gram_right)
    return 1.5 * t - 0.5 * dot(left_of(inner), right_of(t))


def each(count, body):
    if count <= UNROLLED:
        for index in range(count):
            body(index)
    else:
        def loop(index, carry):
            body(index)
            return carry
        lax.fori_loop(0, count, loop, 0)


def totals(gram, seen, step):
    width = gram.shape[0]
    row = lax.broadcasted_iota(jnp.int32, gram.shape, 0)
    column = lane_of(gram)
    square = gram * gram
    diag_part = jnp.where(row == column, square, 0.0)
    off_part = jnp.where((row == column) | (column >= width), 0.0, square)
    off_total = jnp.sum(jnp.sum(off_part, axis=0, keepdims=True), axis=1, keepdims=True)
    diag_total = jnp.sum(jnp.sum(diag_part, axis=0, keepdims=True), axis=1, keepdims=True)
    line = lax.broadcasted_iota(jnp.int32, seen.shape, 0)
    fresh = jnp.where(line == 0, off_total, diag_total)
    return jnp.where((lane_of(seen) == step) & (line < 2), fresh, seen)


def doubled(lanes):
    return lanes // 2 // 256 * 256


def kernel(plan_hbm, columns_ref, out_ref, stat_ref,
           plan_ref, columns, raw, turned, paired, ready, extra_raw, extra, extra_paired, own_turn, quarters, leads, stays, last_turns,
           parts, part_in, part_sums, diags, more_diags, crosses, cross_in, sums, stats,
           plan_sem, fetch_sem, blk_send, blk_recv, row_send, row_recv):
    width, share = columns.shape
    half = width // 2
    count = lax.axis_size("rows")
    others = lax.axis_size("blk")
    me = lax.axis_index("rows")
    mine = lax.axis_index("blk")
    lanes = share // others
    early = lanes // 2 // 128 * 128
    quarter = quarters.shape[2]
    shared = doubled(lanes)
    kept = lanes - shared
    group = others // 2
    base = mine // group * group
    mirror_base = group - base
    place = mine - base
    far_first = sorted(range(1, others), key=lambda offset: (abs(2 * offset - others), offset))

    fetch = pltpu.make_async_copy(columns_ref, columns, fetch_sem)
    fetch.start()
    plan_fetch = pltpu.make_async_copy(plan_hbm, plan_ref, plan_sem)
    plan_fetch.start()
    barrier = pltpu.get_barrier_semaphore()
    for offset in range(1, count):
        pl.semaphore_signal(barrier, inc=1, device_id={"rows": lax.rem(me + offset, count)}, device_id_type=MESH)
    for offset in range(1, others):
        pl.semaphore_signal(barrier, inc=1, device_id={"blk": lax.rem(mine + offset, others)}, device_id_type=MESH)

    def peer_of(offset):
        return lax.rem(mine + offset, others)

    def send(phase, slot, peer, src, dst):
        copy = pltpu.make_async_remote_copy(
            src_ref=src, dst_ref=dst,
            send_sem=blk_send.at[phase, slot], recv_sem=blk_recv.at[phase, slot],
            device_id={"blk": peer}, device_id_type=MESH)
        copy.start()
        return copy

    def blk_copy(phase, offset, src, dst):
        return send(phase, offset - 1, peer_of(offset), src, dst)

    def near_peer(offset):
        return base + lax.rem(place + offset, group)

    def far_peer(offset):
        return mirror_base + lax.rem(place + offset, group)

    far_peers = [(offset, far_peer(offset)) for offset in range(group)]
    near_peers = [(group + offset - 1, near_peer(offset)) for offset in range(1, group)]

    def gather(phase, ref):
        return [blk_copy(phase, offset, ref.at[mine], ref.at[mine]) for offset in far_first]

    def scatter(phase, src_ref, dst_ref):
        return [blk_copy(phase, offset, src_ref.at[peer_of(offset)], dst_ref.at[mine]) for offset in far_first]

    def exchange(phase, peers, src_ref, start, size):
        copies = []
        for slot, peer in peers:
            lane_start = pl.multiple_of(peer * lanes + start, 128)
            copies.append(send(phase, slot, peer, src_ref.at[:, pl.ds(lane_start, size)],
                               raw.at[mine, :, pl.ds(start, size)]))
        return copies

    def finish(copies):
        for copy in copies:
            copy.wait()

    def total_of(ref):
        total = ref[0]
        for index in range(1, ref.shape[0]):
            total = total + ref[index]
        return total

    def share_rows(phase, ref):
        copies = []
        for offset in range(1, count):
            copy = pltpu.make_async_remote_copy(
                src_ref=ref.at[me], dst_ref=ref.at[me],
                send_sem=row_send.at[phase, offset - 1], recv_sem=row_recv.at[phase, offset - 1],
                device_id={"rows": lax.rem(me + offset, count)}, device_id_type=MESH)
            copy.start()
            copies.append(copy)
        return copies

    def start_rows(phase, packed):
        sums[phase, me] = packed
        return share_rows(phase, sums.at[phase])

    def end_rows(phase, copies):
        finish(copies)
        return total_of(sums.at[phase])

    def source(step, slot, pair):
        return lax.rem(pair + others - (plan_ref[step, slot] >> 1), others)

    def partner(step):
        return lax.rem(mine + others - (plan_ref[step, 0] >> 1) - (plan_ref[step, 1] >> 1), others)

    def placed(ref, step, pair, where=slice(None)):
        return jnp.concatenate([ref[source(step, 0, pair), pl.ds(0, half), where],
                                ref[source(step, 1, pair), pl.ds(half, half), where]], axis=0)

    def whole(packed):
        return jnp.concatenate(unpack(packed), axis=0)

    low_lane = (lax.broadcasted_iota(jnp.int32, (half, 2 * width), 1) & (width - 1)) < half
    def rotated_diag(turn, gram, first_leaves):
        rotated = dot_turned(left_of(dot(left_of(turn), right_of(gram))), turned_right_of(turn))
        first, second = rotated[:half], rotated[half:]
        leaving = jnp.where(first_leaves,
                            jnp.where(low_lane, first, pltpu.roll(first, half, 1)),
                            jnp.where(low_lane, pltpu.roll(second, half, 1), second))
        return first, second, pack_block(leaving)

    def spread(more):
        size = shared // 2
        start = kept + more * size
        into = pl.ds(more * size, size)
        copies = []
        for offset in range(1, group):
            peer = near_peer(offset)
            mirrored = mirror_base + peer - base
            lane_start = pl.multiple_of(mirrored * lanes + start, 128)
            copies.append(send(SPREAD + more, offset - 1, peer, columns.at[:, pl.ds(lane_start, size)],
                               extra_raw.at[mine, :, into]))
        copies.append(send(MIRROR + more, 0, mirror_base + place, raw.at[pl.ds(base, group), :, pl.ds(start, size)],
                           extra_raw.at[pl.ds(base, group), :, into]))
        lane_start = pl.multiple_of((mirror_base + place) * lanes + start, 128)
        extra_raw[mine, :, into] = columns[:, pl.ds(lane_start, size)]
        return copies

    pl.semaphore_wait(barrier, count - 1 + others - 1)
    early_copies = exchange(EXCHANGE, far_peers, columns_ref, 0, early) if early else []
    late_copies = exchange(EXCHANGE_LATE, far_peers[:AHEAD], columns_ref, early, lanes - early)
    early_copies += exchange(EXCHANGE, near_peers, columns_ref, 0, early) if early else []
    fetch.wait()
    value = columns[...]
    gram = cross_gram(value, value)
    row_copies = start_rows(0, pack(gram))
    raw[mine] = columns[:, pl.ds(pl.multiple_of(mine * lanes, 128), lanes)]
    plan_fetch.wait()

    gram = whole(end_rows(0, row_copies))
    seen = totals(gram, jnp.zeros(stats.shape[1:], jnp.float32), 0)
    turn = pair_rotation(gram)
    own_turn[...] = pack(turn)
    my_quarter = pl.ds(pl.multiple_of(me * quarter, quarter), quarter)
    turn_copies = [blk_copy(TURN0, offset, own_turn.at[my_quarter], quarters.at[me, mine]) for offset in far_first]
    late_copies += exchange(EXCHANGE_LATE, far_peers[AHEAD:] + near_peers, columns, early, lanes - early)
    first_leaves = (plan_ref[0, 0] >> 1) > 0
    first_diag, second_diag, diags[mine] = rotated_diag(turn, gram, first_leaves)
    quarters[me, mine] = own_turn[my_quarter]
    finish(turn_copies)
    turn_rows = share_rows(ROW_SUMS, quarters)
    finish(turn_rows)

    def first_turn_of(pair):
        return whole(jnp.concatenate([quarters[index, pair] for index in range(count)], axis=0))

    def first_turn(start, size):
        def body(pair):
            where = pl.ds(start, size)
            turned[pair, :, where] = dot(left_of(first_turn_of(pair)), right_of(raw[pair, :, where]))
        each(others, body)

    finish(early_copies)
    if early:
        first_turn(0, early)
    finish(late_copies)
    first_turn(early, lanes - early)

    def pair_gram(pair):
        value = placed(turned, 0, pair)
        paired[pair] = value
        parts[pair] = pack_block(block_cross(value[:half], value[half:]))

    each(others, pair_gram)
    part_copies = scatter(PARTS, parts, part_in)
    diag_copies = gather(DIAG0, diags)
    part_in[mine] = parts[mine]

    def pair_cross(pair):
        crosses[pair] = pack(cross_gram(paired[source(1, 0, pair)], paired[source(1, 1, pair)]))

    each(others, pair_cross)
    cross_in[mine] = crosses[mine]

    finish(part_copies)
    part_sums[me] = total_of(part_in)
    row_copies = share_rows(1, part_sums)
    cross_copies = scatter(CROSS, crosses, cross_in)
    finish(diag_copies)
    from_other = unpack_block(diags[partner(0)], half)
    finish(row_copies)
    block = unpack_block(total_of(part_sums), half)
    gram = jnp.concatenate([
        jnp.where(low_lane, jnp.where(first_leaves, from_other, first_diag), block),
        jnp.where(low_lane, flip_block(block), jnp.where(first_leaves, second_diag, from_other))], axis=0)
    spread_copies = spread(0) if shared else []
    seen = totals(gram, seen, 1)
    turn = pair_rotation(gram)
    first_leaves = (plan_ref[1, 0] >> 1) > 0
    lead = jnp.where(first_leaves, turn[:half], turn[half:])
    stay = jnp.where(first_leaves, turn[half:], turn[:half])
    leads[mine] = pack(lead)
    lead_copies = gather(LEAD1, leads)
    stays[mine] = pack(stay)
    first_diag, second_diag, more_diags[mine] = rotated_diag(turn, gram, first_leaves)
    diag_copies = gather(DIAG1, more_diags)
    finish(cross_copies)
    cross_rows = start_rows(2, total_of(cross_in))
    cross = whole(end_rows(2, cross_rows))
    cross_right, cross_turned = right_of(cross), turned_right_of(cross)
    finish(lead_copies)
    from_other = whole(leads[partner(1)])
    first_turns = jnp.where(first_leaves, from_other, stay)
    second_turns = jnp.where(first_leaves, stay, from_other)
    inner = jnp.concatenate([dot(left_of(first_turns), cross_right),
                             dot_turned(left_of(second_turns), cross_turned)], axis=0)
    outer = dot_turned(left_of(inner), turned_right_of(jnp.concatenate([first_turns, second_turns], axis=0)))
    finish(diag_copies)
    stay_copies = gather(STAY1, stays)
    finish(spread_copies)
    spread_copies = spread(1) if shared else []
    from_other = unpack_block(more_diags[partner(1)], half)
    gram = jnp.concatenate([
        jnp.where(low_lane, jnp.where(first_leaves, from_other, first_diag), outer[:half]),
        jnp.where(low_lane, outer[half:], jnp.where(first_leaves, second_diag, from_other))], axis=0)
    stats[mine] = totals(gram, seen, 2)
    stat_copies = gather(STATS, stats)
    last_turns[mine] = pack(pair_rotation(gram))
    turn_copies = gather(TURN2, last_turns)

    finish(stay_copies)

    def second_turn_of(pair):
        lead, stay = whole(leads[pair]), whole(stays[pair])
        return left_of(jnp.concatenate([jnp.where(first_leaves, lead, stay),
                                        jnp.where(first_leaves, stay, lead)], axis=0))

    def second_turn(pair):
        ready[pair] = dot(second_turn_of(pair), right_of(paired[pair]))

    each(others, second_turn)

    def pair_again(pair):
        paired[pair] = placed(ready, 1, pair)

    each(others, pair_again)
    finish(spread_copies)
    if shared:
        def extra_first(pair):
            extra[pair] = dot(left_of(first_turn_of(pair)), right_of(extra_raw[pair]))

        def extra_pair(pair):
            extra_paired[pair] = placed(extra, 0, pair)

        def extra_second(pair):
            extra_raw[pair] = dot(second_turn_of(pair), right_of(extra_paired[pair]))

        def extra_again(pair):
            extra_paired[pair] = placed(extra_raw, 1, pair)

        each(others, extra_first)
        each(others, extra_pair)
        each(others, extra_second)
        each(others, extra_again)
    finish(stat_copies)
    total = total_of(stats)
    stat_ref[...] = jnp.broadcast_to(jnp.sqrt(total[0:1]) / jnp.sqrt(total[1:2]), stat_ref.shape)
    finish(turn_copies)

    def last_turn(pair, ref, size):
        first, second = source(2, 0, pair), source(2, 1, pair)
        where = pl.ds(0, size)
        upper = dot(left_of(unpack(last_turns[first])[0]), right_of(ref[first, :, where]))
        lower = dot(left_of(unpack(last_turns[second])[1]), right_of(ref[second, :, where]))
        return jnp.concatenate([upper, lower], axis=0)

    def lanes_at(chunk, start, size):
        return pl.ds(pl.multiple_of(chunk * lanes + start, 128), size)

    back = []
    for offset in range(group):
        peer = far_peer(offset)
        turned[peer, :, pl.ds(0, kept)] = last_turn(peer, paired, kept)
        back.append(send(FAR, offset, peer, turned.at[peer, :, pl.ds(0, kept)], out_ref.at[:, lanes_at(mine, 0, kept)]))
    mirror = mirror_base + place
    for offset in list(range(1, group)) + [0]:
        peer = near_peer(offset)
        result = last_turn(peer, paired, lanes)
        if offset:
            turned[peer] = result
            back.append(send(NEAR, offset - 1, peer, turned.at[peer], out_ref.at[:, lanes_at(mine, 0, lanes)]))
        else:
            out_ref[:, lanes_at(mine, 0, lanes)] = result
        if shared:
            result = last_turn(peer, extra_paired, shared)
            if offset:
                extra[peer] = result
                back.append(send(NEAR_MORE, offset - 1, peer, extra.at[peer],
                                 out_ref.at[:, lanes_at(mirror, kept, shared)]))
            else:
                out_ref[:, lanes_at(mirror, kept, shared)] = result
    finish(back)


def place_kernel(current_ref, stat_ref, out_ref, ratio_ref, sems):
    width = current_ref.shape[0]
    pieces = sems.shape[0]
    size = width // pieces
    copies = []
    for index in range(pieces):
        where = pl.ds(index * size, size)
        copy = pltpu.make_async_copy(current_ref.at[where], out_ref.at[where], sems.at[index])
        copy.start()
        copies.append(copy)
    line = lax.broadcasted_iota(jnp.int32, stat_ref.shape, 0)
    values = stat_ref[...]
    for index in range(ratio_ref.shape[0]):
        ratio_ref[index] = jnp.sum(jnp.where((lane_of(values) == index) & (line == 0), values, 0.0))
    for copy in copies:
        copy.wait()


def local(columns, plan):
    width, share = columns.shape
    half = width // 2
    steps = plan.shape[0]
    count = lax.axis_size("rows")
    others = lax.axis_size("blk")
    lanes = share // others
    smem = pl.BlockSpec(memory_space=pltpu.SMEM)
    vmem = pl.BlockSpec(memory_space=pltpu.VMEM)
    hbm = pl.BlockSpec(memory_space=pl.ANY)
    stored = pl.BlockSpec(memory_space=pltpu.HBM)
    wide = pltpu.VMEM((others, width, lanes), jnp.float32)
    more = pltpu.VMEM((others, width, max(doubled(lanes), 128)), jnp.float32)
    small = pltpu.VMEM((others, half, 2 * width), jnp.float32)
    smaller = pltpu.VMEM((others, half // 2, 2 * width), jnp.float32)
    block = pltpu.VMEM((others, half * half // (2 * width), 2 * width), jnp.float32)
    current, stat = pl.pallas_call(
        kernel,
        out_shape=(
            jax.ShapeDtypeStruct(columns.shape, jnp.float32),
            jax.ShapeDtypeStruct((8, 128), jnp.float32),
        ),
        in_specs=[stored, stored],
        out_specs=(vmem, vmem),
        scratch_shapes=[
            pltpu.SMEM(plan.shape, jnp.int32),
            pltpu.VMEM((width, share), jnp.float32),
            wide, wide, wide, wide,
            more, more, more,
            pltpu.VMEM((half, 2 * width), jnp.float32),
            pltpu.VMEM((count, others, half // count, 2 * width), jnp.float32),
            smaller, smaller, small,
            block, block, pltpu.VMEM((count,) + block.shape[1:], jnp.float32), block, block,
            small, small,
            pltpu.VMEM((ROW_SUMS, count, half, 2 * width), jnp.float32),
            pltpu.VMEM((others, 8, 128), jnp.float32),
            pltpu.SemaphoreType.DMA,
            pltpu.SemaphoreType.DMA,
            pltpu.SemaphoreType.DMA((BLK_PHASES, max(others - 1, 1))),
            pltpu.SemaphoreType.DMA((BLK_PHASES, max(others - 1, 1))),
            pltpu.SemaphoreType.DMA((ROW_PHASES, max(count - 1, 1))),
            pltpu.SemaphoreType.DMA((ROW_PHASES, max(count - 1, 1))),
        ],
        compiler_params=pltpu.CompilerParams(collective_id=0, has_side_effects=True, vmem_limit_bytes=55_000_000),
        name="steps",
    )(plan, columns)
    return pl.pallas_call(
        place_kernel,
        out_shape=(
            jax.ShapeDtypeStruct(columns.shape, jnp.float32),
            jax.ShapeDtypeStruct((steps,), jnp.float32),
        ),
        in_specs=[vmem, vmem],
        out_specs=(hbm, smem),
        scratch_shapes=[pltpu.SemaphoreType.DMA((8,))],
        compiler_params=pltpu.CompilerParams(vmem_limit_bytes=8 << 20),
        name="place",
    )(current, stat)


def solution(mesh):
    return jax.shard_map(
        local,
        mesh=mesh,
        in_specs=(P("blk", "rows"), P()),
        out_specs=(P("blk", "rows"), P()),
        check_vma=False,
    )
```

```python
from functools import partial

import jax
import jax.numpy as jnp
from jax import lax
from jax.experimental import pallas as pl
from jax.experimental.pallas import tpu as pltpu
from jax.sharding import PartitionSpec as P

EIG_ITERS = 3
NS_ITERS = 8
UNROLLED = 8
AHEAD = 1
MESH = pl.DeviceIdType.MESH
(EXCHANGE, EXCHANGE_LATE, TURN0, DIAG0, PARTS, CROSS, LEAD1, DIAG1, STAY1, TURN2, STATS,
 SPREAD, SPREAD_MORE, MIRROR, MIRROR_MORE, NEAR, NEAR_MORE, FAR) = range(18)
BLK_PHASES = 18
ROW_SUMS = 3
ROW_PHASES = 4


def split(value):
    high = value.astype(jnp.bfloat16)
    low = (value - high.astype(jnp.float32)).astype(jnp.bfloat16)
    return high, low


def left_of(value):
    high = value.astype(jnp.bfloat16).astype(jnp.float32)
    low = value - high
    lane = lax.broadcasted_iota(jnp.int32, value.shape, 1)
    mixed = jnp.where(lane < value.shape[1] // 2, high, low).astype(jnp.bfloat16)
    return jnp.concatenate([mixed, mixed], axis=1)


def right_of(value):
    high, low = split(value)
    return jnp.concatenate([high, high, low, low], axis=0)


def turned_right_of(value):
    high, low = split(value)
    both = jnp.concatenate([high, low], axis=1)
    return jnp.concatenate([both, both], axis=0)


def dot(left, right):
    return jnp.dot(left, right, preferred_element_type=jnp.float32)


def dot_turned(left, right):
    return lax.dot_general(left, right, (((1,), (1,)), ((), ())), preferred_element_type=jnp.float32)


def cross_gram(first, second):
    width = first.shape[0]
    left = jnp.concatenate(split(first), axis=0)
    right = left if second is first else jnp.concatenate(split(second), axis=0)
    products = dot_turned(left, right)
    folded = products + pltpu.roll(products, width, 1)
    return folded[:width] + folded[width:]


def lane_of(value):
    return lax.broadcasted_iota(jnp.int32, value.shape, 1)


def pack(value):
    half = value.shape[0] // 2
    top = value[:half]
    return jnp.where(lane_of(top) < value.shape[1] // 2, top, value[half:])


def unpack(packed):
    width = packed.shape[1] // 2
    turned = pltpu.roll(packed, width, 1)
    first = lane_of(packed) < width
    return jnp.where(first, packed, turned), jnp.where(first, turned, packed)


def block_cross(first, second):
    half = first.shape[0]
    high, low = split(second)
    right = jnp.concatenate([high, low, high, low], axis=0)
    products = dot_turned(jnp.concatenate(split(first), axis=0), right)
    folded = products + pltpu.roll(products, half, 1)
    return folded[:half] + folded[half:]


def pack_block(value):
    half, across = value.shape
    groups = across // half
    rows = half // groups
    packed = value[:rows]
    for index in range(1, groups):
        packed = jnp.where(lane_of(packed) < index * half, packed, value[index * rows:(index + 1) * rows])
    return packed


def unpack_block(packed, half):
    groups = packed.shape[1] // half
    lane = lane_of(packed)
    rows = []
    for index in range(groups):
        value = jnp.where((lane >= index * half) & (lane < (index + 1) * half), packed, 0.0)
        reach = half
        while reach < packed.shape[1]:
            value = value + pltpu.roll(value, reach, 1)
            reach *= 2
        rows.append(value)
    return jnp.concatenate(rows, axis=0)


def flip_block(value):
    half, across = value.shape
    return jnp.concatenate([value] * (across // half), axis=0).T[:half]


def orthonormal(z, zt, gram_left, gram_right):
    y = z / jnp.sqrt(jnp.sum(z * z, axis=0, keepdims=True))
    t = zt / jnp.sqrt(0.5 * jnp.sum(zt * zt, axis=1, keepdims=True))
    inner = dot(left_of(t), right_of(y))
    bound = jnp.max(jnp.sum(jnp.abs(inner), axis=0, keepdims=True), axis=1, keepdims=True)
    root = jnp.sqrt(bound)
    y = y / root
    t = t / root

    def finish(y, t, inner):
        y_next = 1.5 * y - 0.5 * dot(left_of(y), right_of(inner))
        t_next = 1.5 * t - 0.5 * dot(left_of(inner), right_of(t))
        return y_next, t_next

    y, t = finish(y, t, inner / bound)
    for _ in range(2, NS_ITERS):
        y, t = finish(y, t, dot(left_of(t), right_of(y)))
    inner = dot(left_of(t), right_of(y))
    return y, t, inner, finish(dot(gram_left, right_of(y)), dot(left_of(t), gram_right), inner)


def pair_rotation(gram):
    gram_left, gram_right = left_of(gram), right_of(gram)

    def again(_, carry):
        return orthonormal(*carry, gram_left, gram_right)[3]

    z, zt = lax.fori_loop(1, EIG_ITERS, again, (gram, gram))
    y, t, inner, _ = orthonormal(z, zt, gram_left, gram_right)
    return 1.5 * t - 0.5 * dot(left_of(inner), right_of(t))


def each(count, body):
    if count <= UNROLLED:
        for index in range(count):
            body(index)
    else:
        def loop(index, carry):
            body(index)
            return carry
        lax.fori_loop(0, count, loop, 0)


def totals(gram, seen, step):
    width = gram.shape[0]
    row = lax.broadcasted_iota(jnp.int32, gram.shape, 0)
    column = lane_of(gram)
    square = gram * gram
    diag_part = jnp.where(row == column, square, 0.0)
    off_part = jnp.where((row == column) | (column >= width), 0.0, square)
    off_total = jnp.sum(jnp.sum(off_part, axis=0, keepdims=True), axis=1, keepdims=True)
    diag_total = jnp.sum(jnp.sum(diag_part, axis=0, keepdims=True), axis=1, keepdims=True)
    line = lax.broadcasted_iota(jnp.int32, seen.shape, 0)
    fresh = jnp.where(line == 0, off_total, diag_total)
    return jnp.where((lane_of(seen) == step) & (line < 2), fresh, seen)


def doubled(lanes):
    return lanes // 2 // 256 * 256


def kernel(plan_hbm, columns_ref, out_ref, stat_ref,
           plan_ref, columns, raw, turned, paired, ready, extra_raw, extra, extra_paired, own_turn, quarters, leads, stays, last_turns,
           parts, part_in, part_sums, diags, more_diags, crosses, cross_in, sums, stats,
           plan_sem, fetch_sem, blk_send, blk_recv, row_send, row_recv):
    width, share = columns.shape
    half = width // 2
    count = lax.axis_size("rows")
    others = lax.axis_size("blk")
    me = lax.axis_index("rows")
    mine = lax.axis_index("blk")
    lanes = share // others
    early = lanes // 2 // 128 * 128
    quarter = quarters.shape[2]
    shared = doubled(lanes)
    kept = lanes - shared
    group = others // 2
    base = mine // group * group
    mirror_base = group - base
    place = mine - base
    far_first = sorted(range(1, others), key=lambda offset: (abs(2 * offset - others), offset))

    fetch = pltpu.make_async_copy(columns_ref, columns, fetch_sem)
    fetch.start()
    plan_fetch = pltpu.make_async_copy(plan_hbm, plan_ref, plan_sem)
    plan_fetch.start()
    barrier = pltpu.get_barrier_semaphore()
    for offset in range(1, count):
        pl.semaphore_signal(barrier, inc=1, device_id={"rows": lax.rem(me + offset, count)}, device_id_type=MESH)
    for offset in range(1, others):
        pl.semaphore_signal(barrier, inc=1, device_id={"blk": lax.rem(mine + offset, others)}, device_id_type=MESH)

    def peer_of(offset):
        return lax.rem(mine + offset, others)

    def send(phase, slot, peer, src, dst):
        copy = pltpu.make_async_remote_copy(
            src_ref=src, dst_ref=dst,
            send_sem=blk_send.at[phase, slot], recv_sem=blk_recv.at[phase, slot],
            device_id={"blk": peer}, device_id_type=MESH)
        copy.start()
        return copy

    def blk_copy(phase, offset, src, dst):
        return send(phase, offset - 1, peer_of(offset), src, dst)

    def near_peer(offset):
        return base + lax.rem(place + offset, group)

    def far_peer(offset):
        return mirror_base + lax.rem(place + offset, group)

    far_peers = [(offset, far_peer(offset)) for offset in range(group)]
    near_peers = [(group + offset - 1, near_peer(offset)) for offset in range(1, group)]

    def gather(phase, ref):
        return [blk_copy(phase, offset, ref.at[mine], ref.at[mine]) for offset in far_first]

    def scatter(phase, src_ref, dst_ref):
        return [blk_copy(phase, offset, src_ref.at[peer_of(offset)], dst_ref.at[mine]) for offset in far_first]

    def exchange(phase, peers, src_ref, start, size):
        copies = []
        for slot, peer in peers:
            lane_start = pl.multiple_of(peer * lanes + start, 128)
            copies.append(send(phase, slot, peer, src_ref.at[:, pl.ds(lane_start, size)],
                               raw.at[mine, :, pl.ds(start, size)]))
        return copies

    def finish(copies):
        for copy in copies:
            copy.wait()

    def total_of(ref):
        total = ref[0]
        for index in range(1, ref.shape[0]):
            total = total + ref[index]
        return total

    def share_rows(phase, ref):
        copies = []
        for offset in range(1, count):
            copy = pltpu.make_async_remote_copy(
                src_ref=ref.at[me], dst_ref=ref.at[me],
                send_sem=row_send.at[phase, offset - 1], recv_sem=row_recv.at[phase, offset - 1],
                device_id={"rows": lax.rem(me + offset, count)}, device_id_type=MESH)
            copy.start()
            copies.append(copy)
        return copies

    def start_rows(phase, packed):
        sums[phase, me] = packed
        return share_rows(phase, sums.at[phase])

    def end_rows(phase, copies):
        finish(copies)
        return total_of(sums.at[phase])

    def source(step, slot, pair):
        return lax.rem(pair + others - (plan_ref[step, slot] >> 1), others)

    def partner(step):
        return lax.rem(mine + others - (plan_ref[step, 0] >> 1) - (plan_ref[step, 1] >> 1), others)

    def placed(ref, step, pair, where=slice(None)):
        return jnp.concatenate([ref[source(step, 0, pair), pl.ds(0, half), where],
                                ref[source(step, 1, pair), pl.ds(half, half), where]], axis=0)

    def whole(packed):
        return jnp.concatenate(unpack(packed), axis=0)

    low_lane = (lax.broadcasted_iota(jnp.int32, (half, 2 * width), 1) & (width - 1)) < half
    def rotated_diag(turn, gram, first_leaves):
        rotated = dot_turned(left_of(dot(left_of(turn), right_of(gram))), turned_right_of(turn))
        first, second = rotated[:half], rotated[half:]
        leaving = jnp.where(first_leaves,
                            jnp.where(low_lane, first, pltpu.roll(first, half, 1)),
                            jnp.where(low_lane, pltpu.roll(second, half, 1), second))
        return first, second, pack_block(leaving)

    def spread(more):
        size = shared // 2
        start = kept + more * size
        into = pl.ds(more * size, size)
        copies = []
        for offset in range(1, group):
            peer = near_peer(offset)
            mirrored = mirror_base + peer - base
            lane_start = pl.multiple_of(mirrored * lanes + start, 128)
            copies.append(send(SPREAD + more, offset - 1, peer, columns.at[:, pl.ds(lane_start, size)],
                               extra_raw.at[mine, :, into]))
        copies.append(send(MIRROR + more, 0, mirror_base + place, raw.at[pl.ds(base, group), :, pl.ds(start, size)],
                           extra_raw.at[pl.ds(base, group), :, into]))
        lane_start = pl.multiple_of((mirror_base + place) * lanes + start, 128)
        extra_raw[mine, :, into] = columns[:, pl.ds(lane_start, size)]
        return copies

    pl.semaphore_wait(barrier, count - 1 + others - 1)
    early_copies = exchange(EXCHANGE, far_peers, columns_ref, 0, early) if early else []
    late_copies = exchange(EXCHANGE_LATE, far_peers[:AHEAD], columns_ref, early, lanes - early)
    early_copies += exchange(EXCHANGE, near_peers, columns_ref, 0, early) if early else []
    fetch.wait()
    value = columns[...]
    gram = cross_gram(value, value)
    row_copies = start_rows(0, pack(gram))
    raw[mine] = columns[:, pl.ds(pl.multiple_of(mine * lanes, 128), lanes)]
    plan_fetch.wait()

    gram = whole(end_rows(0, row_copies))
    seen = totals(gram, jnp.zeros(stats.shape[1:], jnp.float32), 0)
    turn = pair_rotation(gram)
    own_turn[...] = pack(turn)
    my_quarter = pl.ds(pl.multiple_of(me * quarter, quarter), quarter)
    turn_copies = [blk_copy(TURN0, offset, own_turn.at[my_quarter], quarters.at[me, mine]) for offset in far_first]
    late_copies += exchange(EXCHANGE_LATE, far_peers[AHEAD:] + near_peers, columns, early, lanes - early)
    first_leaves = (plan_ref[0, 0] >> 1) > 0
    first_diag, second_diag, diags[mine] = rotated_diag(turn, gram, first_leaves)
    quarters[me, mine] = own_turn[my_quarter]
    finish(turn_copies)
    turn_rows = share_rows(ROW_SUMS, quarters)
    finish(turn_rows)

    def first_turn_of(pair):
        return whole(jnp.concatenate([quarters[index, pair] for index in range(count)], axis=0))

    def first_turn(start, size):
        def body(pair):
            where = pl.ds(start, size)
            turned[pair, :, where] = dot(left_of(first_turn_of(pair)), right_of(raw[pair, :, where]))
        each(others, body)

    finish(early_copies)
    if early:
        first_turn(0, early)
    finish(late_copies)
    first_turn(early, lanes - early)

    def pair_gram(pair):
        value = placed(turned, 0, pair)
        paired[pair] = value
        parts[pair] = pack_block(block_cross(value[:half], value[half:]))

    each(others, pair_gram)
    part_copies = scatter(PARTS, parts, part_in)
    diag_copies = gather(DIAG0, diags)
    part_in[mine] = parts[mine]

    def pair_cross(pair):
        crosses[pair] = pack(cross_gram(paired[source(1, 0, pair)], paired[source(1, 1, pair)]))

    each(others, pair_cross)
    cross_in[mine] = crosses[mine]

    finish(part_copies)
    part_sums[me] = total_of(part_in)
    row_copies = share_rows(1, part_sums)
    cross_copies = scatter(CROSS, crosses, cross_in)
    finish(diag_copies)
    from_other = unpack_block(diags[partner(0)], half)
    finish(row_copies)
    block = unpack_block(total_of(part_sums), half)
    gram = jnp.concatenate([
        jnp.where(low_lane, jnp.where(first_leaves, from_other, first_diag), block),
        jnp.where(low_lane, flip_block(block), jnp.where(first_leaves, second_diag, from_other))], axis=0)
    spread_copies = spread(0) if shared else []
    seen = totals(gram, seen, 1)
    turn = pair_rotation(gram)
    first_leaves = (plan_ref[1, 0] >> 1) > 0
    lead = jnp.where(first_leaves, turn[:half], turn[half:])
    stay = jnp.where(first_leaves, turn[half:], turn[:half])
    leads[mine] = pack(lead)
    lead_copies = gather(LEAD1, leads)
    stays[mine] = pack(stay)
    first_diag, second_diag, more_diags[mine] = rotated_diag(turn, gram, first_leaves)
    diag_copies = gather(DIAG1, more_diags)
    finish(cross_copies)
    cross_rows = start_rows(2, total_of(cross_in))
    cross = whole(end_rows(2, cross_rows))
    cross_right, cross_turned = right_of(cross), turned_right_of(cross)
    finish(lead_copies)
    from_other = whole(leads[partner(1)])
    first_turns = jnp.where(first_leaves, from_other, stay)
    second_turns = jnp.where(first_leaves, stay, from_other)
    inner = jnp.concatenate([dot(left_of(first_turns), cross_right),
                             dot_turned(left_of(second_turns), cross_turned)], axis=0)
    outer = dot_turned(left_of(inner), turned_right_of(jnp.concatenate([first_turns, second_turns], axis=0)))
    finish(diag_copies)
    stay_copies = gather(STAY1, stays)
    finish(spread_copies)
    spread_copies = spread(1) if shared else []
    from_other = unpack_block(more_diags[partner(1)], half)
    gram = jnp.concatenate([
        jnp.where(low_lane, jnp.where(first_leaves, from_other, first_diag), outer[:half]),
        jnp.where(low_lane, outer[half:], jnp.where(first_leaves, second_diag, from_other))], axis=0)
    stats[mine] = totals(gram, seen, 2)
    stat_copies = gather(STATS, stats)
    last_turns[mine] = pack(pair_rotation(gram))
    turn_copies = gather(TURN2, last_turns)

    finish(stay_copies)

    def second_turn_of(pair):
        lead, stay = whole(leads[pair]), whole(stays[pair])
        return left_of(jnp.concatenate([jnp.where(first_leaves, lead, stay),
                                        jnp.where(first_leaves, stay, lead)], axis=0))

    def second_turn(pair):
        ready[pair] = dot(second_turn_of(pair), right_of(paired[pair]))

    each(others, second_turn)

    def pair_again(pair):
        paired[pair] = placed(ready, 1, pair)

    each(others, pair_again)
    finish(spread_copies)
    if shared:
        def extra_first(pair):
            extra[pair] = dot(left_of(first_turn_of(pair)), right_of(extra_raw[pair]))

        def extra_pair(pair):
            extra_paired[pair] = placed(extra, 0, pair)

        def extra_second(pair):
            extra_raw[pair] = dot(second_turn_of(pair), right_of(extra_paired[pair]))

        def extra_again(pair):
            extra_paired[pair] = placed(extra_raw, 1, pair)

        each(others, extra_first)
        each(others, extra_pair)
        each(others, extra_second)
        each(others, extra_again)
    finish(stat_copies)
    total = total_of(stats)
    stat_ref[...] = jnp.broadcast_to(jnp.sqrt(total[0:1]) / jnp.sqrt(total[1:2]), stat_ref.shape)
    finish(turn_copies)

    def last_turn(pair, ref, size):
        first, second = source(2, 0, pair), source(2, 1, pair)
        where = pl.ds(0, size)
        upper = dot(left_of(unpack(last_turns[first])[0]), right_of(ref[first, :, where]))
        lower = dot(left_of(unpack(last_turns[second])[1]), right_of(ref[second, :, where]))
        return jnp.concatenate([upper, lower], axis=0)

    def lanes_at(chunk, start, size):
        return pl.ds(pl.multiple_of(chunk * lanes + start, 128), size)

    back = []
    for offset in range(group):
        peer = far_peer(offset)
        turned[peer, :, pl.ds(0, kept)] = last_turn(peer, paired, kept)
        back.append(send(FAR, offset, peer, turned.at[peer, :, pl.ds(0, kept)], out_ref.at[:, lanes_at(mine, 0, kept)]))
    mirror = mirror_base + place
    for offset in list(range(1, group)) + [0]:
        peer = near_peer(offset)
        result = last_turn(peer, paired, lanes)
        if offset:
            turned[peer] = result
            back.append(send(NEAR, offset - 1, peer, turned.at[peer], out_ref.at[:, lanes_at(mine, 0, lanes)]))
        else:
            out_ref[:, lanes_at(mine, 0, lanes)] = result
        if shared:
            result = last_turn(peer, extra_paired, shared)
            if offset:
                extra[peer] = result
                back.append(send(NEAR_MORE, offset - 1, peer, extra.at[peer],
                                 out_ref.at[:, lanes_at(mirror, kept, shared)]))
            else:
                out_ref[:, lanes_at(mirror, kept, shared)] = result
    finish(back)


def place_kernel(current_ref, stat_ref, out_ref, ratio_ref, sems):
    width = current_ref.shape[0]
    pieces = sems.shape[0]
    size = width // pieces
    copies = []
    for index in range(pieces):
        where = pl.ds(index * size, size)
        copy = pltpu.make_async_copy(current_ref.at[where], out_ref.at[where], sems.at[index])
        copy.start()
        copies.append(copy)
    line = lax.broadcasted_iota(jnp.int32, stat_ref.shape, 0)
    values = stat_ref[...]
    for index in range(ratio_ref.shape[0]):
        ratio_ref[index] = jnp.sum(jnp.where((lane_of(values) == index) & (line == 0), values, 0.0))
    for copy in copies:
        copy.wait()


def local(columns, plan):
    width, share = columns.shape
    half = width // 2
    steps = plan.shape[0]
    count = lax.axis_size("rows")
    others = lax.axis_size("blk")
    lanes = share // others
    smem = pl.BlockSpec(memory_space=pltpu.SMEM)
    vmem = pl.BlockSpec(memory_space=pltpu.VMEM)
    hbm = pl.BlockSpec(memory_space=pl.ANY)
    stored = pl.BlockSpec(memory_space=pltpu.HBM)
    wide = pltpu.VMEM((others, width, lanes), jnp.float32)
    more = pltpu.VMEM((others, width, max(doubled(lanes), 128)), jnp.float32)
    small = pltpu.VMEM((others, half, 2 * width), jnp.float32)
    smaller = pltpu.VMEM((others, half // 2, 2 * width), jnp.float32)
    block = pltpu.VMEM((others, half * half // (2 * width), 2 * width), jnp.float32)
    current, stat = pl.pallas_call(
        kernel,
        out_shape=(
            jax.ShapeDtypeStruct(columns.shape, jnp.float32),
            jax.ShapeDtypeStruct((8, 128), jnp.float32),
        ),
        in_specs=[stored, stored],
        out_specs=(vmem, vmem),
        scratch_shapes=[
            pltpu.SMEM(plan.shape, jnp.int32),
            pltpu.VMEM((width, share), jnp.float32),
            wide, wide, wide, wide,
            more, more, more,
            pltpu.VMEM((half, 2 * width), jnp.float32),
            pltpu.VMEM((count, others, half // count, 2 * width), jnp.float32),
            smaller, smaller, small,
            block, block, pltpu.VMEM((count,) + block.shape[1:], jnp.float32), block, block,
            small, small,
            pltpu.VMEM((ROW_SUMS, count, half, 2 * width), jnp.float32),
            pltpu.VMEM((others, 8, 128), jnp.float32),
            pltpu.SemaphoreType.DMA,
            pltpu.SemaphoreType.DMA,
            pltpu.SemaphoreType.DMA((BLK_PHASES, max(others - 1, 1))),
            pltpu.SemaphoreType.DMA((BLK_PHASES, max(others - 1, 1))),
            pltpu.SemaphoreType.DMA((ROW_PHASES, max(count - 1, 1))),
            pltpu.SemaphoreType.DMA((ROW_PHASES, max(count - 1, 1))),
        ],
        compiler_params=pltpu.CompilerParams(collective_id=0, has_side_effects=True, vmem_limit_bytes=55_000_000),
        name="steps",
    )(pltpu.with_memory_space_constraint(plan, pltpu.HBM), columns)
    return pl.pallas_call(
        place_kernel,
        out_shape=(
            jax.ShapeDtypeStruct(columns.shape, jnp.float32),
            jax.ShapeDtypeStruct((steps,), jnp.float32),
        ),
        in_specs=[vmem, vmem],
        out_specs=(hbm, smem),
        scratch_shapes=[pltpu.SemaphoreType.DMA((8,))],
        compiler_params=pltpu.CompilerParams(vmem_limit_bytes=8 << 20),
        name="place",
    )(current, stat)


def solution(mesh):
    return jax.shard_map(
        local,
        mesh=mesh,
        in_specs=(P("blk", "rows"), P()),
        out_specs=(P("blk", "rows"), P()),
        check_vma=False,
    )
```

```python
from functools import partial

import jax
import jax.numpy as jnp
from jax import lax
from jax.experimental import pallas as pl
from jax.experimental.pallas import tpu as pltpu
from jax.sharding import PartitionSpec as P

EIG_ITERS = 3
NS_ITERS = 8
UNROLLED = 8
AHEAD = 1
MESH = pl.DeviceIdType.MESH
(EXCHANGE, EXCHANGE_LATE, TURN0, DIAG0, PARTS, CROSS, LEAD1, DIAG1, STAY1, TURN2, STATS,
 SPREAD, SPREAD_MORE, MIRROR, MIRROR_MORE, NEAR, NEAR_MORE, FAR) = range(18)
BLK_PHASES = 18
ROW_SUMS = 3
ROW_PHASES = 4


def split(value):
    high = value.astype(jnp.bfloat16)
    low = (value - high.astype(jnp.float32)).astype(jnp.bfloat16)
    return high, low


def left_of(value):
    high = value.astype(jnp.bfloat16).astype(jnp.float32)
    low = value - high
    lane = lax.broadcasted_iota(jnp.int32, value.shape, 1)
    mixed = jnp.where(lane < value.shape[1] // 2, high, low).astype(jnp.bfloat16)
    return jnp.concatenate([mixed, mixed], axis=1)


def right_of(value):
    high, low = split(value)
    return jnp.concatenate([high, high, low, low], axis=0)


def turned_right_of(value):
    high, low = split(value)
    both = jnp.concatenate([high, low], axis=1)
    return jnp.concatenate([both, both], axis=0)


def dot(left, right):
    return jnp.dot(left, right, preferred_element_type=jnp.float32)


def dot_turned(left, right):
    return lax.dot_general(left, right, (((1,), (1,)), ((), ())), preferred_element_type=jnp.float32)


def cross_gram(first, second):
    width = first.shape[0]
    left = jnp.concatenate(split(first), axis=0)
    right = left if second is first else jnp.concatenate(split(second), axis=0)
    products = dot_turned(left, right)
    folded = products + pltpu.roll(products, width, 1)
    return folded[:width] + folded[width:]


def lane_of(value):
    return lax.broadcasted_iota(jnp.int32, value.shape, 1)


def pack(value):
    half = value.shape[0] // 2
    top = value[:half]
    return jnp.where(lane_of(top) < value.shape[1] // 2, top, value[half:])


def unpack(packed):
    width = packed.shape[1] // 2
    turned = pltpu.roll(packed, width, 1)
    first = lane_of(packed) < width
    return jnp.where(first, packed, turned), jnp.where(first, turned, packed)


def block_cross(first, second):
    half = first.shape[0]
    high, low = split(second)
    right = jnp.concatenate([high, low, high, low], axis=0)
    products = dot_turned(jnp.concatenate(split(first), axis=0), right)
    folded = products + pltpu.roll(products, half, 1)
    return folded[:half] + folded[half:]


def pack_block(value):
    half, across = value.shape
    groups = across // half
    rows = half // groups
    packed = value[:rows]
    for index in range(1, groups):
        packed = jnp.where(lane_of(packed) < index * half, packed, value[index * rows:(index + 1) * rows])
    return packed


def unpack_block(packed, half):
    groups = packed.shape[1] // half
    lane = lane_of(packed)
    rows = []
    for index in range(groups):
        value = jnp.where((lane >= index * half) & (lane < (index + 1) * half), packed, 0.0)
        reach = half
        while reach < packed.shape[1]:
            value = value + pltpu.roll(value, reach, 1)
            reach *= 2
        rows.append(value)
    return jnp.concatenate(rows, axis=0)


def flip_block(value):
    half, across = value.shape
    return jnp.concatenate([value] * (across // half), axis=0).T[:half]


def orthonormal(z, zt, gram_left, gram_right):
    y = z / jnp.sqrt(jnp.sum(z * z, axis=0, keepdims=True))
    t = zt / jnp.sqrt(0.5 * jnp.sum(zt * zt, axis=1, keepdims=True))
    inner = dot(left_of(t), right_of(y))
    bound = jnp.max(jnp.sum(jnp.abs(inner), axis=0, keepdims=True), axis=1, keepdims=True)
    root = jnp.sqrt(bound)
    y = y / root
    t = t / root

    def finish(y, t, inner):
        y_next = 1.5 * y - 0.5 * dot(left_of(y), right_of(inner))
        t_next = 1.5 * t - 0.5 * dot(left_of(inner), right_of(t))
        return y_next, t_next

    y, t = finish(y, t, inner / bound)
    for _ in range(2, NS_ITERS):
        y, t = finish(y, t, dot(left_of(t), right_of(y)))
    inner = dot(left_of(t), right_of(y))
    return y, t, inner, finish(dot(gram_left, right_of(y)), dot(left_of(t), gram_right), inner)


def pair_rotation(gram):
    gram_left, gram_right = left_of(gram), right_of(gram)

    def again(_, carry):
        return orthonormal(*carry, gram_left, gram_right)[3]

    z, zt = lax.fori_loop(1, EIG_ITERS, again, (gram, gram))
    y, t, inner, _ = orthonormal(z, zt, gram_left, gram_right)
    return 1.5 * t - 0.5 * dot(left_of(inner), right_of(t))


def each(count, body):
    if count <= UNROLLED:
        for index in range(count):
            body(index)
    else:
        def loop(index, carry):
            body(index)
            return carry
        lax.fori_loop(0, count, loop, 0)


def totals(gram, seen, step):
    width = gram.shape[0]
    row = lax.broadcasted_iota(jnp.int32, gram.shape, 0)
    column = lane_of(gram)
    square = gram * gram
    diag_part = jnp.where(row == column, square, 0.0)
    off_part = jnp.where((row == column) | (column >= width), 0.0, square)
    off_total = jnp.sum(jnp.sum(off_part, axis=0, keepdims=True), axis=1, keepdims=True)
    diag_total = jnp.sum(jnp.sum(diag_part, axis=0, keepdims=True), axis=1, keepdims=True)
    line = lax.broadcasted_iota(jnp.int32, seen.shape, 0)
    fresh = jnp.where(line == 0, off_total, diag_total)
    return jnp.where((lane_of(seen) == step) & (line < 2), fresh, seen)


def doubled(lanes):
    return lanes // 2 // 256 * 256


def kernel(plan_hbm, columns_ref, out_ref, stat_ref,
           plan_ref, columns, raw, turned, paired, ready, extra_raw, extra, extra_paired, own_turn, quarters, leads, stays, last_turns,
           parts, part_in, part_sums, diags, more_diags, crosses, cross_in, sums, stats,
           plan_sem, fetch_sem, blk_send, blk_recv, row_send, row_recv):
    width, share = columns.shape
    half = width // 2
    count = lax.axis_size("rows")
    others = lax.axis_size("blk")
    me = lax.axis_index("rows")
    mine = lax.axis_index("blk")
    lanes = share // others
    early = lanes // 2 // 128 * 128
    quarter = quarters.shape[2]
    shared = doubled(lanes)
    kept = lanes - shared
    group = others // 2
    base = mine // group * group
    mirror_base = group - base
    place = mine - base
    far_first = sorted(range(1, others), key=lambda offset: (abs(2 * offset - others), offset))

    fetch = pltpu.make_async_copy(columns_ref, columns, fetch_sem)
    fetch.start()
    plan_fetch = pltpu.make_async_copy(plan_hbm, plan_ref, plan_sem)
    plan_fetch.start()
    barrier = pltpu.get_barrier_semaphore()
    for offset in range(1, count):
        pl.semaphore_signal(barrier, inc=1, device_id={"rows": lax.rem(me + offset, count)}, device_id_type=MESH)
    for offset in range(1, others):
        pl.semaphore_signal(barrier, inc=1, device_id={"blk": lax.rem(mine + offset, others)}, device_id_type=MESH)

    def peer_of(offset):
        return lax.rem(mine + offset, others)

    def send(phase, slot, peer, src, dst):
        copy = pltpu.make_async_remote_copy(
            src_ref=src, dst_ref=dst,
            send_sem=blk_send.at[phase, slot], recv_sem=blk_recv.at[phase, slot],
            device_id={"blk": peer}, device_id_type=MESH)
        copy.start()
        return copy

    def blk_copy(phase, offset, src, dst):
        return send(phase, offset - 1, peer_of(offset), src, dst)

    def near_peer(offset):
        return base + lax.rem(place + offset, group)

    def far_peer(offset):
        return mirror_base + lax.rem(place + offset, group)

    far_peers = [(offset, far_peer(offset)) for offset in range(group)]
    near_peers = [(group + offset - 1, near_peer(offset)) for offset in range(1, group)]

    def gather(phase, ref):
        return [blk_copy(phase, offset, ref.at[mine], ref.at[mine]) for offset in far_first]

    def scatter(phase, src_ref, dst_ref):
        return [blk_copy(phase, offset, src_ref.at[peer_of(offset)], dst_ref.at[mine]) for offset in far_first]

    def exchange(phase, peers, src_ref, start, size):
        copies = []
        for slot, peer in peers:
            lane_start = pl.multiple_of(peer * lanes + start, 128)
            copies.append(send(phase, slot, peer, src_ref.at[:, pl.ds(lane_start, size)],
                               raw.at[mine, :, pl.ds(start, size)]))
        return copies

    def finish(copies):
        for copy in copies:
            copy.wait()

    def total_of(ref):
        total = ref[0]
        for index in range(1, ref.shape[0]):
            total = total + ref[index]
        return total

    def share_rows(phase, ref):
        copies = []
        for offset in range(1, count):
            copy = pltpu.make_async_remote_copy(
                src_ref=ref.at[me], dst_ref=ref.at[me],
                send_sem=row_send.at[phase, offset - 1], recv_sem=row_recv.at[phase, offset - 1],
                device_id={"rows": lax.rem(me + offset, count)}, device_id_type=MESH)
            copy.start()
            copies.append(copy)
        return copies

    def start_rows(phase, packed):
        sums[phase, me] = packed
        return share_rows(phase, sums.at[phase])

    def end_rows(phase, copies):
        finish(copies)
        return total_of(sums.at[phase])

    def source(step, slot, pair):
        return lax.rem(pair + others - (plan_ref[step, slot] >> 1), others)

    def partner(step):
        return lax.rem(mine + others - (plan_ref[step, 0] >> 1) - (plan_ref[step, 1] >> 1), others)

    def placed(ref, step, pair, where=slice(None)):
        return jnp.concatenate([ref[source(step, 0, pair), pl.ds(0, half), where],
                                ref[source(step, 1, pair), pl.ds(half, half), where]], axis=0)

    def whole(packed):
        return jnp.concatenate(unpack(packed), axis=0)

    low_lane = (lax.broadcasted_iota(jnp.int32, (half, 2 * width), 1) & (width - 1)) < half
    def rotated_diag(turn, gram, first_leaves):
        rotated = dot_turned(left_of(dot(left_of(turn), right_of(gram))), turned_right_of(turn))
        first, second = rotated[:half], rotated[half:]
        leaving = jnp.where(first_leaves,
                            jnp.where(low_lane, first, pltpu.roll(first, half, 1)),
                            jnp.where(low_lane, pltpu.roll(second, half, 1), second))
        return first, second, pack_block(leaving)

    def spread(more):
        size = shared // 2
        start = kept + more * size
        into = pl.ds(more * size, size)
        copies = []
        copies.append(send(MIRROR + more, 0, mirror_base + place, raw.at[pl.ds(base, group), :, pl.ds(start, size)],
                           extra_raw.at[pl.ds(base, group), :, into]))
        for offset in range(1, group):
            peer = near_peer(offset)
            mirrored = mirror_base + peer - base
            lane_start = pl.multiple_of(mirrored * lanes + start, 128)
            copies.append(send(SPREAD + more, offset - 1, peer, columns.at[:, pl.ds(lane_start, size)],
                               extra_raw.at[mine, :, into]))
        lane_start = pl.multiple_of((mirror_base + place) * lanes + start, 128)
        extra_raw[mine, :, into] = columns[:, pl.ds(lane_start, size)]
        return copies

    pl.semaphore_wait(barrier, count - 1 + others - 1)
    early_copies = exchange(EXCHANGE, far_peers, columns_ref, 0, early) if early else []
    late_copies = exchange(EXCHANGE_LATE, far_peers[:AHEAD], columns_ref, early, lanes - early)
    early_copies += exchange(EXCHANGE, near_peers, columns_ref, 0, early) if early else []
    fetch.wait()
    value = columns[...]
    gram = cross_gram(value, value)
    row_copies = start_rows(0, pack(gram))
    raw[mine] = columns[:, pl.ds(pl.multiple_of(mine * lanes, 128), lanes)]
    plan_fetch.wait()

    gram = whole(end_rows(0, row_copies))
    seen = totals(gram, jnp.zeros(stats.shape[1:], jnp.float32), 0)
    turn = pair_rotation(gram)
    own_turn[...] = pack(turn)
    my_quarter = pl.ds(pl.multiple_of(me * quarter, quarter), quarter)
    turn_copies = [blk_copy(TURN0, offset, own_turn.at[my_quarter], quarters.at[me, mine]) for offset in far_first]
    late_copies += exchange(EXCHANGE_LATE, far_peers[AHEAD:] + near_peers, columns, early, lanes - early)
    first_leaves = (plan_ref[0, 0] >> 1) > 0
    first_diag, second_diag, diags[mine] = rotated_diag(turn, gram, first_leaves)
    quarters[me, mine] = own_turn[my_quarter]
    finish(turn_copies)
    turn_rows = share_rows(ROW_SUMS, quarters)
    finish(turn_rows)

    def first_turn_of(pair):
        return whole(jnp.concatenate([quarters[index, pair] for index in range(count)], axis=0))

    def first_turn(start, size):
        def body(pair):
            where = pl.ds(start, size)
            turned[pair, :, where] = dot(left_of(first_turn_of(pair)), right_of(raw[pair, :, where]))
        each(others, body)

    finish(early_copies)
    if early:
        first_turn(0, early)
    finish(late_copies)
    first_turn(early, lanes - early)

    def pair_gram(pair):
        value = placed(turned, 0, pair)
        paired[pair] = value
        parts[pair] = pack_block(block_cross(value[:half], value[half:]))

    each(others, pair_gram)
    part_copies = scatter(PARTS, parts, part_in)
    diag_copies = gather(DIAG0, diags)
    part_in[mine] = parts[mine]

    def pair_cross(pair):
        crosses[pair] = pack(cross_gram(paired[source(1, 0, pair)], paired[source(1, 1, pair)]))

    each(others, pair_cross)
    cross_in[mine] = crosses[mine]

    finish(part_copies)
    part_sums[me] = total_of(part_in)
    row_copies = share_rows(1, part_sums)
    cross_copies = scatter(CROSS, crosses, cross_in)
    finish(diag_copies)
    from_other = unpack_block(diags[partner(0)], half)
    finish(row_copies)
    block = unpack_block(total_of(part_sums), half)
    gram = jnp.concatenate([
        jnp.where(low_lane, jnp.where(first_leaves, from_other, first_diag), block),
        jnp.where(low_lane, flip_block(block), jnp.where(first_leaves, second_diag, from_other))], axis=0)
    spread_copies = spread(0) if shared else []
    seen = totals(gram, seen, 1)
    turn = pair_rotation(gram)
    first_leaves = (plan_ref[1, 0] >> 1) > 0
    lead = jnp.where(first_leaves, turn[:half], turn[half:])
    stay = jnp.where(first_leaves, turn[half:], turn[:half])
    leads[mine] = pack(lead)
    lead_copies = gather(LEAD1, leads)
    stays[mine] = pack(stay)
    first_diag, second_diag, more_diags[mine] = rotated_diag(turn, gram, first_leaves)
    diag_copies = gather(DIAG1, more_diags)
    finish(cross_copies)
    cross_rows = start_rows(2, total_of(cross_in))
    cross = whole(end_rows(2, cross_rows))
    cross_right, cross_turned = right_of(cross), turned_right_of(cross)
    finish(lead_copies)
    from_other = whole(leads[partner(1)])
    first_turns = jnp.where(first_leaves, from_other, stay)
    second_turns = jnp.where(first_leaves, stay, from_other)
    inner = jnp.concatenate([dot(left_of(first_turns), cross_right),
                             dot_turned(left_of(second_turns), cross_turned)], axis=0)
    outer = dot_turned(left_of(inner), turned_right_of(jnp.concatenate([first_turns, second_turns], axis=0)))
    finish(diag_copies)
    stay_copies = gather(STAY1, stays)
    spread_copies += spread(1) if shared else []
    from_other = unpack_block(more_diags[partner(1)], half)
    gram = jnp.concatenate([
        jnp.where(low_lane, jnp.where(first_leaves, from_other, first_diag), outer[:half]),
        jnp.where(low_lane, outer[half:], jnp.where(first_leaves, second_diag, from_other))], axis=0)
    stats[mine] = totals(gram, seen, 2)
    stat_copies = gather(STATS, stats)
    last_turns[mine] = pack(pair_rotation(gram))
    turn_copies = gather(TURN2, last_turns)

    finish(stay_copies)

    def second_turn_of(pair):
        lead, stay = whole(leads[pair]), whole(stays[pair])
        return left_of(jnp.concatenate([jnp.where(first_leaves, lead, stay),
                                        jnp.where(first_leaves, stay, lead)], axis=0))

    def second_turn(pair):
        ready[pair] = dot(second_turn_of(pair), right_of(paired[pair]))

    each(others, second_turn)

    def pair_again(pair):
        paired[pair] = placed(ready, 1, pair)

    each(others, pair_again)
    finish(spread_copies)
    if shared:
        def extra_first(pair):
            extra[pair] = dot(left_of(first_turn_of(pair)), right_of(extra_raw[pair]))

        def extra_pair(pair):
            extra_paired[pair] = placed(extra, 0, pair)

        def extra_second(pair):
            extra_raw[pair] = dot(second_turn_of(pair), right_of(extra_paired[pair]))

        def extra_again(pair):
            extra_paired[pair] = placed(extra_raw, 1, pair)

        each(others, extra_first)
        each(others, extra_pair)
        each(others, extra_second)
        each(others, extra_again)
    finish(stat_copies)
    total = total_of(stats)
    stat_ref[...] = jnp.broadcast_to(jnp.sqrt(total[0:1]) / jnp.sqrt(total[1:2]), stat_ref.shape)
    finish(turn_copies)

    def last_turn(pair, ref, size):
        first, second = source(2, 0, pair), source(2, 1, pair)
        where = pl.ds(0, size)
        upper = dot(left_of(unpack(last_turns[first])[0]), right_of(ref[first, :, where]))
        lower = dot(left_of(unpack(last_turns[second])[1]), right_of(ref[second, :, where]))
        return jnp.concatenate([upper, lower], axis=0)

    def lanes_at(chunk, start, size):
        return pl.ds(pl.multiple_of(chunk * lanes + start, 128), size)

    back = []
    for offset in range(group):
        peer = far_peer(offset)
        turned[peer, :, pl.ds(0, kept)] = last_turn(peer, paired, kept)
        back.append(send(FAR, offset, peer, turned.at[peer, :, pl.ds(0, kept)], out_ref.at[:, lanes_at(mine, 0, kept)]))
    mirror = mirror_base + place
    for offset in list(range(1, group)) + [0]:
        peer = near_peer(offset)
        result = last_turn(peer, paired, lanes)
        if offset:
            turned[peer] = result
            back.append(send(NEAR, offset - 1, peer, turned.at[peer], out_ref.at[:, lanes_at(mine, 0, lanes)]))
        else:
            out_ref[:, lanes_at(mine, 0, lanes)] = result
        if shared:
            result = last_turn(peer, extra_paired, shared)
            if offset:
                extra[peer] = result
                back.append(send(NEAR_MORE, offset - 1, peer, extra.at[peer],
                                 out_ref.at[:, lanes_at(mirror, kept, shared)]))
            else:
                out_ref[:, lanes_at(mirror, kept, shared)] = result
    finish(back)


def place_kernel(current_ref, stat_ref, out_ref, ratio_ref, sems):
    width = current_ref.shape[0]
    pieces = sems.shape[0]
    size = width // pieces
    copies = []
    for index in range(pieces):
        where = pl.ds(index * size, size)
        copy = pltpu.make_async_copy(current_ref.at[where], out_ref.at[where], sems.at[index])
        copy.start()
        copies.append(copy)
    line = lax.broadcasted_iota(jnp.int32, stat_ref.shape, 0)
    values = stat_ref[...]
    for index in range(ratio_ref.shape[0]):
        ratio_ref[index] = jnp.sum(jnp.where((lane_of(values) == index) & (line == 0), values, 0.0))
    for copy in copies:
        copy.wait()


def local(columns, plan):
    width, share = columns.shape
    half = width // 2
    steps = plan.shape[0]
    count = lax.axis_size("rows")
    others = lax.axis_size("blk")
    lanes = share // others
    smem = pl.BlockSpec(memory_space=pltpu.SMEM)
    vmem = pl.BlockSpec(memory_space=pltpu.VMEM)
    hbm = pl.BlockSpec(memory_space=pl.ANY)
    stored = pl.BlockSpec(memory_space=pltpu.HBM)
    wide = pltpu.VMEM((others, width, lanes), jnp.float32)
    more = pltpu.VMEM((others, width, max(doubled(lanes), 128)), jnp.float32)
    small = pltpu.VMEM((others, half, 2 * width), jnp.float32)
    smaller = pltpu.VMEM((others, half // 2, 2 * width), jnp.float32)
    block = pltpu.VMEM((others, half * half // (2 * width), 2 * width), jnp.float32)
    current, stat = pl.pallas_call(
        kernel,
        out_shape=(
            jax.ShapeDtypeStruct(columns.shape, jnp.float32),
            jax.ShapeDtypeStruct((8, 128), jnp.float32),
        ),
        in_specs=[stored, stored],
        out_specs=(vmem, vmem),
        scratch_shapes=[
            pltpu.SMEM(plan.shape, jnp.int32),
            pltpu.VMEM((width, share), jnp.float32),
            wide, wide, wide, wide,
            more, more, more,
            pltpu.VMEM((half, 2 * width), jnp.float32),
            pltpu.VMEM((count, others, half // count, 2 * width), jnp.float32),
            smaller, smaller, small,
            block, block, pltpu.VMEM((count,) + block.shape[1:], jnp.float32), block, block,
            small, small,
            pltpu.VMEM((ROW_SUMS, count, half, 2 * width), jnp.float32),
            pltpu.VMEM((others, 8, 128), jnp.float32),
            pltpu.SemaphoreType.DMA,
            pltpu.SemaphoreType.DMA,
            pltpu.SemaphoreType.DMA((BLK_PHASES, max(others - 1, 1))),
            pltpu.SemaphoreType.DMA((BLK_PHASES, max(others - 1, 1))),
            pltpu.SemaphoreType.DMA((ROW_PHASES, max(count - 1, 1))),
            pltpu.SemaphoreType.DMA((ROW_PHASES, max(count - 1, 1))),
        ],
        compiler_params=pltpu.CompilerParams(collective_id=0, has_side_effects=True, vmem_limit_bytes=55_000_000),
        name="steps",
    )(pltpu.with_memory_space_constraint(plan, pltpu.HBM), columns)
    return pl.pallas_call(
        place_kernel,
        out_shape=(
            jax.ShapeDtypeStruct(columns.shape, jnp.float32),
            jax.ShapeDtypeStruct((steps,), jnp.float32),
        ),
        in_specs=[vmem, vmem],
        out_specs=(hbm, smem),
        scratch_shapes=[pltpu.SemaphoreType.DMA((8,))],
        compiler_params=pltpu.CompilerParams(vmem_limit_bytes=8 << 20),
        name="place",
    )(current, stat)


def solution(mesh):
    return jax.shard_map(
        local,
        mesh=mesh,
        in_specs=(P("blk", "rows"), P()),
        out_specs=(P("blk", "rows"), P()),
        check_vma=False,
    )
```
